512 devices in a mesh: row: 16 (over x, y), col: 32 (over z, core).
Axes of the slice: x: 4, y: 4, z: 16, core: 2. Of those that a mesh axis runs over, the one named last changes fastest.
Arguments:
- arrival: float32 [64, 16384], P(None, 'col'), may hold values from 0 to 4
- delay: bfloat16 [4, 16384, 16384], P(None, 'col', 'row'), may hold values from -40 to 20
- occupancy: int32 [4, 32, 32], replicated, may hold values from 0 to 1, as said below
Outputs:
- final_arrival: float32 [64, 16384], P(None, 'col')
- worst: float32 [64], replicated
The draws below stay inside these ranges and needn't reach their ends.
Inputs may be any that keep to these rules, and one draw needn't show every extreme that they name: In every level every column of tiles holds at least one tile with occupancy 1.
All inputs are finite; a program needn't handle non-finite values.
Results may differ from the reference program's by a relative error of at most 0.0009.
Values sent between devices are 32-bit elements; how exact they have to be, the bound alone decides.
A program may use at most 64 MiB of HBM per device.

```python
import jax
import jax.numpy as jnp
from jax import lax

TILE = 512
SCEN = 64
LEVELS = 4
TILES = 32
PINS = 16384


def draw_occupancy(key, part):
    first, second = jax.random.split(jax.random.fold_in(key, 7))
    base = jax.random.randint(first, (LEVELS, TILES, TILES), 0, 2, dtype=jnp.int32)
    picked = jax.random.randint(second, (LEVELS, 1, TILES), 0, TILES, dtype=jnp.int32)
    places = jnp.arange(TILES, dtype=jnp.int32)[None, :, None]
    forced = (places == picked).astype(jnp.int32)
    return jnp.maximum(base, forced)


def draw_delay(key, part):
    spread = jnp.float32(2.5)
    nominal = spread * jnp.sqrt(2.0 * jnp.log(jnp.float32(0.5 * PINS)))
    first, second, third = jax.random.split(jax.random.fold_in(key, 11), 3)
    normal_part = jnp.clip(jax.random.normal(first, (LEVELS, PINS, PINS), jnp.float32), -6.0, 6.0)
    values = spread * normal_part - nominal
    return jnp.clip(values, -40.0, 20.0).astype(jnp.bfloat16)


def levels(rng, shape, pieces, smallest, high):
    level, own = 1.0, jax.random.fold_in(rng, 6)
    for dim, parts in pieces:
        heights = jnp.exp(jax.random.uniform(jax.random.fold_in(own, dim), (parts,), jnp.float32, smallest / len(pieces), high / len(pieces)))
        level = level * jnp.repeat(heights, shape[dim] // parts).reshape([-1 if axis == dim else 1 for axis in range(len(shape))])
    return level


def setup_inputs(seed: int = 0) -> dict:
    key_list = jax.random.split(jax.random.key(seed), 4)
    return {
        "arrival": jnp.clip(4.0 * jax.random.uniform(key_list[0], (SCEN, PINS), jnp.float32) ** levels(key_list[0], (SCEN, PINS), ((1, 32),), -0.2, 0.2), 0.0, 4.0),
        "delay": draw_delay(jax.random.fold_in(key_list[3], 71), 0),
        "occupancy": draw_occupancy(jax.random.fold_in(key_list[3], 71), 0),
    }


def level_max(times, delay_level, flags):
    width = min(32, TILE)
    turns = PINS // width

    def step(best, index):
        start = (index * width).astype(jnp.int32)
        part_a = lax.dynamic_slice_in_dim(times, start, width, 1)
        part_d = lax.dynamic_slice_in_dim(delay_level, start, width, 0).astype(jnp.float32)
        tile_row = lax.dynamic_index_in_dim(flags, (start // TILE).astype(jnp.int32), 0, keepdims=False)
        keep = jnp.repeat(tile_row > 0, TILE)
        masked = jnp.where(keep[None, :], part_d, jnp.float32(-1e9))
        return jnp.maximum(best, jnp.max(part_a[:, :, None] + masked[None, :, :], axis=1)), None

    init = jnp.full((times.shape[0], PINS), -1e9, jnp.float32)
    best, unused = lax.scan(step, init, jnp.arange(turns, dtype=jnp.int32))
    return best


def reference(arrival, delay, occupancy):
    times = arrival
    for level in range(LEVELS):
        times = level_max(times, delay[level], occupancy[level])
    return times, jnp.max(times, axis=1)
```

```python
import functools

import jax
import jax.numpy as jnp
from jax import lax
from jax.experimental import pallas as pl
from jax.experimental.pallas import tpu as pltpu
from jax.sharding import PartitionSpec as P

MESH = pl.DeviceIdType.MESH
NEG = -1000000000.0
GROUPS = 4
OWNERS = 4
LATE = 1
EARLY = 2


def kernel(
    arrival_ref, occ_ref, delay_ref,
    final_ref, worst_ref,
    raw, dmat, part, inbox, times, wbox, wown,
    raw_sem, part_send, part_recv, gath_send, gath_recv, w_send, w_recv,
):
    levels, tile, width = delay_ref.shape
    row = lax.axis_index("row")
    col = lax.axis_index("col")
    plane = col // 2
    core = lax.rem(col, 2)
    rows = 16
    cols = 32
    ups = times.shape[3]
    side = rows // OWNERS
    lane_tiles = tile // 128
    is_owner = lax.rem(row, side) == lax.rem(plane, side)
    is_root = row == plane
    slot = row // side

    fetches = [
        pltpu.make_async_copy(delay_ref.at[k], raw.at[k], raw_sem.at[k]) for k in range(levels)
    ]
    for fetch in fetches:
        fetch.start()

    barrier = pltpu.get_barrier_semaphore()

    def greet(to_row, to_col):
        @pl.when(jnp.logical_or(to_row != row, to_col != col))
        def _():
            pl.semaphore_signal(
                barrier, inc=1, device_id={"row": to_row, "col": to_col}, device_id_type=MESH
            )

    @pl.loop(0, 2 * OWNERS)
    def _(n):
        greet((n // 2) * side + lax.rem(row, side), 2 * row + lax.rem(n, 2))

    @pl.when(is_owner)
    def _():
        @pl.loop(0, cols)
        def _(n):
            greet(plane, n)

    @pl.loop(0, rows)
    def _(n):
        greet(n, col)

    @pl.loop(0, cols)
    def _(n):
        greet(row, n)

    def meet():
        extra = jnp.where(is_owner, jnp.where(is_root, cols - 2, cols), 0)
        pl.semaphore_wait(barrier, rows - 1 + cols - 1 + 2 * OWNERS + extra)

    def load_arrival():
        for g in range(GROUPS):
            for l in range(lane_tiles):
                for u in range(ups):
                    s = (g * ups + u) * 8
                    times[0, g, l, u] = arrival_ref[s : s + 8, l * 128 : (l + 1) * 128]

    def decode(k):
        pltpu.make_async_copy(delay_ref.at[k], raw.at[k], raw_sem.at[k]).wait()
        for h in range(2):
            keep = occ_ref[k, col, 2 * row + h] > 0

            @pl.loop(0, tile // 32)
            def _(n):
                at = pl.ds(pl.multiple_of(n * 32, 32), 32)
                for j in range(lane_tiles):
                    lanes = pl.ds(h * tile + j * 128, 128)
                    value = raw[k, at, lanes].astype(jnp.float32)
                    dmat[lax.rem(k, 2), h, j, at, :] = jnp.where(keep, value, jnp.float32(NEG))

    def send_part(k, g, h):
        @pl.when(jnp.logical_and(is_root, h == core))
        def _():
            inbox[k, g, col] = part[k, g, h, slot]

        @pl.loop(0, OWNERS)
        def _(o):
            to_row = o * side + lax.rem(row, side)
            to_col = 2 * row + h

            @pl.when(jnp.logical_or(to_row != row, to_col != col))
            def _():
                pltpu.make_async_remote_copy(
                    src_ref=part.at[k, g, h, o],
                    dst_ref=inbox.at[k, g, col],
                    send_sem=part_send.at[k, g],
                    recv_sem=part_recv.at[k, g],
                    device_id={"row": to_row, "col": to_col},
                    device_id_type=MESH,
                ).start()

    def compute(k, g, send):
        here = lax.rem(k, 2)

        @pl.loop(0, 2)
        def _(h):
            def chunk(l, best):
                best = list(best)
                t = [times[k, g, l, u] for u in range(ups)]
                start = pl.multiple_of(l * 128, 128)
                for i in range(128):
                    d = [
                        dmat[here, h, j, pl.ds(start + i, 8, stride=0), :]
                        for j in range(lane_tiles)
                    ]
                    for u in range(ups):
                        wide = jnp.broadcast_to(t[u][:, i : i + 1], (8, 128))
                        for j in range(lane_tiles):
                            n = u * lane_tiles + j
                            best[n] = jnp.maximum(best[n], wide + d[j])
                return tuple(best)

            init = tuple(jnp.full((8, 128), NEG, jnp.float32) for _ in range(ups * lane_tiles))
            best = lax.fori_loop(0, lane_tiles, chunk, init)
            for u in range(ups):
                for j in range(lane_tiles):
                    part[k, g, h, j, u] = best[u * lane_tiles + j]
            if send:
                send_part(k, g, h)

    def wait_bytes(ref, sem):
        pltpu.make_async_copy(ref, ref, sem).wait()

    def combine(k, g):
        @pl.when(is_owner)
        def _():
            @pl.when(is_root)
            def _():
                wait_bytes(inbox.at[k, g, pl.ds(0, cols - 1)], part_recv.at[k, g])

            @pl.when(jnp.logical_not(is_root))
            def _():
                wait_bytes(inbox.at[k, g], part_recv.at[k, g])

            for u in range(ups):
                tiles = [inbox[k, g, c, u] for c in range(cols)]
                while len(tiles) > 1:
                    tiles = [jnp.maximum(a, b) for a, b in zip(tiles[::2], tiles[1::2])]
                times[k + 1, g, slot, u] = tiles[0]

            @pl.loop(0, rows)
            def _(p):
                @pl.when(p != row)
                def _():
                    pltpu.make_async_remote_copy(
                        src_ref=times.at[k + 1, g, slot],
                        dst_ref=times.at[k + 1, g, slot],
                        send_sem=gath_send.at[k, g],
                        recv_sem=gath_recv.at[k, g],
                        device_id={"row": p, "col": col},
                        device_id_type=MESH,
                    ).start()

    def take(k, g):
        @pl.when(is_owner)
        def _():
            wait_bytes(times.at[k + 1, g, pl.ds(0, OWNERS - 1)], gath_recv.at[k, g])

        @pl.when(jnp.logical_not(is_owner))
        def _():
            wait_bytes(times.at[k + 1, g], gath_recv.at[k, g])

    load_arrival()
    decode(0)

    @pl.loop(0, EARLY)
    def _(g):
        compute(0, g, False)

    meet()

    @pl.loop(0, EARLY)
    def _(g):
        for h in range(2):
            send_part(0, g, h)

    @pl.loop(0, levels)
    def _(k):
        for g in range(GROUPS):
            @pl.when(k > 0)
            def _():
                if g == 0:
                    for n in range(GROUPS - LATE):
                        combine(k - 1, n)
                elif g <= LATE:
                    combine(k - 1, GROUPS - LATE + g - 1)
                take(k - 1, g)

            if g < EARLY:
                @pl.when(k > 0)
                def _():
                    compute(k, g, True)
            else:
                compute(k, g, True)

        @pl.when(k + 1 < levels)
        def _():
            decode(k + 1)

    for g in range(GROUPS):
        combine(levels - 1, g)
    lane = lax.broadcasted_iota(jnp.int32, (8, 128), 1)
    sub = lax.broadcasted_iota(jnp.int32, (8, 128), 0)
    low = jnp.float32(-3e38)
    spread = jnp.full((8, 128), low, jnp.float32)
    for g in range(GROUPS):
        take(levels - 1, g)
        for u in range(ups):
            n = g * ups + u
            s = n * 8
            tiles = [times[levels, g, l, u] for l in range(lane_tiles)]
            for l in range(lane_tiles):
                final_ref[s : s + 8, l * 128 : (l + 1) * 128] = tiles[l]
            top = functools.reduce(jnp.maximum, tiles)
            top = jnp.max(top, axis=1, keepdims=True)
            spread = jnp.where(lane // 8 == n, top, spread)
    spread = jnp.where(lax.rem(lane, 8) == sub, spread, low)
    spread = jnp.broadcast_to(jnp.max(spread, axis=0, keepdims=True), (8, 128))
    wown[...] = spread
    wbox[col] = spread

    @pl.loop(0, cols)
    def _(n):
        @pl.when(n != col)
        def _():
            pltpu.make_async_remote_copy(
                src_ref=wown,
                dst_ref=wbox.at[col],
                send_sem=w_send,
                recv_sem=w_recv,
                device_id={"row": row, "col": n},
                device_id_type=MESH,
            ).start()

    wait_bytes(wbox.at[pl.ds(0, cols - 1)], w_recv)
    tiles = [wbox[c] for c in range(cols)]
    worst_ref[...] = functools.reduce(jnp.maximum, tiles)

    wait_bytes(wbox.at[pl.ds(0, cols - 1)], w_send)

    @pl.loop(0, levels)
    def _(k):
        for g in range(GROUPS):
            @pl.when(is_root)
            def _():
                wait_bytes(inbox.at[k, g, pl.ds(0, 2 * OWNERS - 1)], part_send.at[k, g])

            @pl.when(jnp.logical_not(is_root))
            def _():
                wait_bytes(inbox.at[k, g, pl.ds(0, 2 * OWNERS)], part_send.at[k, g])

            @pl.when(is_owner)
            def _():
                wait_bytes(inbox.at[k, g, pl.ds(0, rows - 1)], gath_send.at[k, g])


def shards(arrival, delay, occupancy):
    levels, tile, width = delay.shape
    scenarios = arrival.shape[0]
    ups = scenarios // 8 // GROUPS
    lane_tiles = tile // 128
    cols = 32
    vmem = pl.BlockSpec(memory_space=pltpu.VMEM)
    final, worst = pl.pallas_call(
        kernel,
        out_shape=(
            jax.ShapeDtypeStruct((scenarios, tile), jnp.float32),
            jax.ShapeDtypeStruct((8, 128), jnp.float32),
        ),
        in_specs=[vmem, pl.BlockSpec(memory_space=pltpu.SMEM), pl.BlockSpec(memory_space=pl.ANY)],
        out_specs=(vmem, vmem),
        scratch_shapes=[
            pltpu.VMEM((levels, tile, width), jnp.bfloat16),
            pltpu.VMEM((2, 2, lane_tiles, tile, 128), jnp.float32),
            pltpu.VMEM((levels, GROUPS, 2, lane_tiles, ups, 8, 128), jnp.float32),
            pltpu.VMEM((levels, GROUPS, cols, ups, 8, 128), jnp.float32),
            pltpu.VMEM((levels + 1, GROUPS, lane_tiles, ups, 8, 128), jnp.float32),
            pltpu.VMEM((cols, 8, 128), jnp.float32),
            pltpu.VMEM((8, 128), jnp.float32),
            pltpu.SemaphoreType.DMA((levels,)),
            pltpu.SemaphoreType.DMA((levels, GROUPS)),
            pltpu.SemaphoreType.DMA((levels, GROUPS)),
            pltpu.SemaphoreType.DMA((levels, GROUPS)),
            pltpu.SemaphoreType.DMA((levels, GROUPS)),
            pltpu.SemaphoreType.DMA,
            pltpu.SemaphoreType.DMA,
        ],
        compiler_params=pltpu.CompilerParams(collective_id=0, has_side_effects=True),
    )(arrival, occupancy, delay)
    return final, worst[0, :scenarios]


def solution(mesh):
    placed = (P(None, "col"), P(None, "col", "row"), P())
    return jax.shard_map(
        shards, mesh=mesh, in_specs=placed, out_specs=(P(None, "col"), P()), check_vma=False
    )
```
